32 devices in a mesh: rows: 8 (over z, x), feat: 4 (over y, core).
Axes of the slice: x: 2, y: 2, z: 4, core: 2. Of those that a mesh axis runs over, the one named last changes fastest.
Arguments:
- tile_values: bfloat16 [2048, 256, 128], P('rows', 'feat'), may hold values from -6 to 6
- tile_blocks: int32 [2048, 256], P('rows', 'feat'), may hold values from 0 to 2047
- tile_counts: int32 [2048, 4], P('rows', 'feat'), may hold values from 1 to 64, as said below
- labels: int32 [2048], P('rows'), may hold values 0 or 1
- owner_rank: int32 [2048], P('rows'), may hold values from 0 to 7, as said below
- weights: float32 [8192, 128], P(('feat', 'rows')), may hold values from -0.09375 to 0.09375
Outputs:
- owned_margins: float32 [2048], P('rows')
- gradient: float32 [8192, 128], P(('feat', 'rows'))
- loss: float32 [], replicated
The draws below stay inside these ranges and needn't reach their ends.
Inputs may be any that keep to these rules, and one draw needn't show every extreme that they name: `owner_rank`: within each aligned block of 256 examples, every owner is named by exactly 32 examples. `tile_counts`: in every aligned block of 256 examples, each shard's column holds at least one example with exactly 64 used slots.
All inputs are finite; a program needn't handle non-finite values. No bound on the sum of `labels` on one device may be relied on, other than what follows from the above.
Results may differ from the reference program's by a relative error of at most 0.003.
Values may be sent and summed in bfloat16 or wider, within the bound.
A program may use at most 64 MiB of HBM per device.

```python
import jax
import jax.numpy as jnp
from jax import lax

TILE = 128
EX_DEV = 256
TPAD = 64
EXAMPLES = 2048
SLOTS = 256
NBLK = 8192
BLK_SHARD = 2048
PER_PEER = 32
N_ROWS = 8
N_FEAT = 4


def draw_tile_counts(key, part):
    device_count = EXAMPLES // EX_DEV
    shard_count = SLOTS // TPAD
    key_shift = jax.random.fold_in(key, 11)
    key_value = jax.random.fold_in(key, 12)
    key_full = jax.random.fold_in(key, 13)
    device_of = jnp.arange(EXAMPLES, dtype=jnp.int32) // EX_DEV
    spread = max(device_count - 1, 1)
    ceiling = TPAD * (spread + 2 * device_of) // (3 * spread)
    ceiling = jnp.maximum(ceiling, 1)
    shifts = jax.random.randint(key_shift, (EXAMPLES, shard_count), 0, 4)
    divisor = jnp.left_shift(jnp.ones_like(shifts), shifts)
    upper = jnp.maximum(ceiling[:, None] // divisor, 1)
    raw_value = jax.random.randint(key_value, (EXAMPLES, shard_count), 0, 1048576)
    drawn = raw_value % upper + 1
    chosen = jax.random.randint(key_full, (device_count, shard_count), 0, EX_DEV)
    local_index = jnp.arange(EXAMPLES, dtype=jnp.int32) % EX_DEV
    marked = local_index[:, None] == jnp.repeat(chosen, EX_DEV, axis=0)
    return jnp.where(marked, TPAD, drawn).astype(jnp.int32)


def one_block_owner(block_key):
    return jax.random.permutation(block_key, EX_DEV)


def draw_owner_rank(key, part):
    device_count = EXAMPLES // EX_DEV
    block_keys = jax.random.split(jax.random.fold_in(key, 21), device_count)
    shuffled = jax.vmap(one_block_owner)(block_keys)
    return (shuffled // PER_PEER).reshape(EXAMPLES).astype(jnp.int32)


def set_ends(values, key, smallest, high):
    extent = values.shape
    place = [jax.random.randint(jax.random.fold_in(key, axis), (), 0, extent[axis]) for axis in range(len(extent))]
    values = values.at[tuple(place)].set(smallest)
    longest = extent.index(max(extent))
    place[longest] = (place[longest] + 1) % extent[longest]
    return values.at[tuple(place)].set(high)


def levels(rng, dims, pieces, smallest, largest):
    def one(dim, blocks):
        draws = jax.random.uniform(jax.random.fold_in(jax.random.fold_in(rng, 6), dim), (blocks,), jnp.float32, smallest / len(pieces), largest / len(pieces))
        return jnp.repeat(jnp.exp(draws), dims[dim] // blocks).reshape((-1,) + (1,) * (len(dims) - dim - 1))

    factor_of = one(*pieces[0])
    for cut in pieces[1:]:
        factor_of = factor_of * one(*cut)
    return factor_of


def bell_draw(stream_key, dims, width, bound, cuts=(), held_as=jnp.bfloat16):
    loudness = levels(stream_key, dims, cuts, -0.22, 0.18) if cuts else 1.0
    array = jax.random.normal(stream_key, dims, jnp.float32) * width * loudness
    return jnp.minimum(jnp.maximum(array, -bound), bound).astype(held_as)


def setup_inputs(seed: int = 0) -> dict:
    splits = jax.random.split(jax.random.key(seed), 7)
    return {
        "tile_values": bell_draw(splits[0], (EXAMPLES, SLOTS, TILE), 1.0, 6.0, ((0, 8), (1, 4))),
        "tile_blocks": set_ends(jax.random.randint(splits[1], (EXAMPLES, SLOTS), 0, BLK_SHARD), jax.random.fold_in(splits[1], 1), 0, BLK_SHARD - 1).astype(jnp.int32),
        "tile_counts": draw_tile_counts(jax.random.fold_in(splits[6], 71), 0),
        "labels": set_ends((jax.random.randint(splits[3], (EXAMPLES,), 0, 2) < 1).astype(jnp.int32), jax.random.fold_in(splits[3], 1), 0, 1),
        "owner_rank": draw_owner_rank(jax.random.fold_in(splits[6], 71), 0),
        "weights": bell_draw(splits[5], (NBLK, TILE), (TPAD * TPAD) ** -0.5, 0.09375, ((0, 32),), jnp.float32),
    }


def reference(tile_values, tile_blocks, tile_counts, labels, owner_rank, weights):
    w_half = weights.astype(jnp.bfloat16)
    slot_index = jnp.arange(TPAD, dtype=jnp.int32)

    def shard_pieces(shard_index):
        values = lax.dynamic_slice_in_dim(tile_values, shard_index * TPAD, TPAD, 1)
        block_ids = lax.dynamic_slice_in_dim(tile_blocks, shard_index * TPAD, TPAD, 1)
        used = lax.dynamic_slice_in_dim(tile_counts, shard_index, 1, 1)
        live_slot = slot_index[None, :] < used
        return values, block_ids, live_slot

    def shard_margin(shard_index):
        values, block_ids, live_slot = shard_pieces(shard_index)
        weight_table = lax.dynamic_slice_in_dim(w_half, shard_index * BLK_SHARD, BLK_SHARD, 0)
        picked = weight_table[block_ids]
        products = jnp.sum(values.astype(jnp.float32) * picked.astype(jnp.float32), axis=2)
        return jnp.sum(jnp.where(live_slot, products, jnp.float32(0.0)), axis=1)

    shard_index_all = jnp.arange(N_FEAT, dtype=jnp.int32)
    partials = lax.map(shard_margin, shard_index_all)
    margin = jnp.sum(partials, axis=0)
    label_float = labels.astype(jnp.float32)
    residual = jax.nn.sigmoid(margin) - label_float
    loss = jnp.sum(jax.nn.softplus(margin) - label_float * margin) / EXAMPLES
    resid_half = residual.astype(jnp.bfloat16)

    def shard_gradient(shard_index):
        values, block_ids, live_slot = shard_pieces(shard_index)
        coefficient = jnp.where(live_slot, resid_half[:, None], jnp.zeros((), jnp.bfloat16))
        weighted = values.astype(jnp.float32) * coefficient.astype(jnp.float32)[:, :, None]
        return jax.ops.segment_sum(weighted.reshape(-1, TILE), block_ids.reshape(-1), num_segments=BLK_SHARD)

    gradient = lax.map(shard_gradient, shard_index_all).reshape(NBLK, TILE)
    owners = owner_rank.reshape(N_ROWS, EX_DEV)
    send_order = jnp.argsort(owners, axis=1, stable=True).astype(jnp.int32)
    source = send_order + (jnp.arange(N_ROWS, dtype=jnp.int32) * EX_DEV)[:, None]
    source = jnp.transpose(source.reshape(N_ROWS, N_ROWS, PER_PEER), (1, 0, 2)).reshape(EXAMPLES)
    owned_margins = margin[source]
    return owned_margins, gradient, loss
```

```python
import functools

import jax
import jax.numpy as jnp
from jax import lax
from jax.experimental import pallas as pl
from jax.experimental.pallas import tpu as pltpu
from jax.sharding import PartitionSpec as P

MESH = pl.DeviceIdType.MESH
LANES = 128
GRAIN = 16
GROUP = 16
CHUNK = 256
NT = (((1,), (1,)), ((), ()))
NN = (((1,), (0,)), ((), ()))
VM = pl.BlockSpec(memory_space=pltpu.VMEM)
SM = pl.BlockSpec(memory_space=pltpu.SMEM)


def greet(axis, count):
    me = lax.axis_index(axis)
    barrier = pltpu.get_barrier_semaphore()
    for k in range(1, count):
        peer = lax.rem(me + k, count)
        pl.semaphore_signal(barrier, inc=1, device_id={axis: peer}, device_id_type=MESH)
    pl.semaphore_wait(barrier, count - 1)
    return me


def gather_kernel(n, w_ref, table_ref, half, send, recv):
    rows = w_ref.shape[0]
    half[...] = w_ref[...].astype(jnp.bfloat16)
    me = greet("rows", n)
    here = pl.ds(pl.multiple_of(me * rows, rows), rows)
    copies = []
    for k in range(1, n):
        copy = pltpu.make_async_remote_copy(
            src_ref=half,
            dst_ref=table_ref.at[here],
            send_sem=send.at[k - 1],
            recv_sem=recv.at[k - 1],
            device_id={"rows": lax.rem(me + k, n)},
            device_id_type=MESH,
        )
        copy.start()
        copies.append(copy)
    table_ref[here, :] = w_ref[...].astype(jnp.bfloat16)
    for copy in copies:
        copy.wait()


def lane_group():
    return lax.broadcasted_iota(jnp.int32, (1, LANES), 1) // GRAIN


def group_values(vals_ref, glist, base):
    return jnp.concatenate([vals_ref[glist[base + i]] for i in range(GROUP)], axis=0)


def group_offsets(idt, rlist, base):
    group = lane_group()
    per = LANES // GRAIN
    parts = []
    for h in range(GROUP // per):
        row = idt[pl.ds(rlist[base + h * per], 1), :]
        for i in range(1, per):
            row = jnp.where(group == i, idt[pl.ds(rlist[base + h * per + i], 1), :], row)
        parts.append(row)
    ids = jnp.concatenate(parts, axis=1)
    width = GROUP * GRAIN
    return jnp.broadcast_to(ids, (8, width)) - lax.broadcasted_iota(jnp.int32, (8, width), 0)


def margin_kernel(counts, used_ref, ids_ref, table_ref, vals_ref, glist, rlist, nb, idt, partial_ref, terms):
    ex, slots = ids_ref.shape
    grains = slots // GRAIN
    live = lax.broadcasted_iota(jnp.int32, (ex, slots), 1) < used_ref[...]
    shifted = jnp.where(live, ids_ref[...] + 1, 0)
    if slots < LANES:
        shifted = jnp.concatenate([shifted, jnp.zeros((ex, LANES - slots), jnp.int32)], axis=1)
    lane = lax.broadcasted_iota(jnp.int32, (ex, LANES), 1) // GRAIN
    for q in range(grains):
        piece = jnp.where(lane == q, shifted, 0)
        step = GRAIN
        while step < LANES:
            piece = piece + pltpu.roll(piece, step, 1)
            step *= 2
        idt[q * ex : (q + 1) * ex, :] = piece - 1
    idt[grains * ex :, :] = jnp.full((8, LANES), -1, jnp.int32)

    def fill(e, off):
        for q in range(grains):
            glist[off + q] = e * grains + q
            rlist[off + q] = e + q * ex
        return off + (counts[e] + (GRAIN - 1)) // GRAIN

    total = lax.fori_loop(0, ex, fill, jnp.int32(0), unroll=8)
    for i in range(GROUP):
        glist[total + i] = 0
        rlist[total + i] = grains * ex
    turns = (total + (GROUP - 1)) // GROUP
    nb[0] = turns
    terms[...] = jnp.zeros_like(terms)
    group = lane_group()
    width = GROUP * GRAIN
    per = LANES // GRAIN

    def turn(t, carry):
        base = t * GROUP
        values = group_values(vals_ref, glist, base)
        offset = group_offsets(idt, rlist, base)
        found = jnp.zeros((8, width), jnp.float32)
        for c in range(table_ref.shape[0] // CHUNK):
            scores = lax.dot_general(
                table_ref[c * CHUNK : (c + 1) * CHUNK, :], values, NT, preferred_element_type=jnp.float32
            )
            for i in range(CHUNK // 8):
                found = jnp.where(offset == c * CHUNK + i * 8, scores[i * 8 : i * 8 + 8, :], found)
        term = jnp.sum(found, axis=0, keepdims=True)
        for i in range(GROUP):
            h = i // per
            mine = jnp.where(group == i % per, term[:, h * LANES : (h + 1) * LANES], 0.0)
            terms[pl.ds(rlist[base + i], 1), :] = mine
        return carry

    lax.fori_loop(0, turns, turn, jnp.int32(0))
    spread = terms[0:ex, :]
    for q in range(1, grains):
        spread = spread + terms[q * ex : (q + 1) * ex, :]
    partial_ref[...] = jnp.broadcast_to(jnp.sum(spread.T, axis=0, keepdims=True), partial_ref.shape)


def residual_kernel(n, partial_ref, labels_ref, margin_ref, resid_ref, loss_ref, held, send, recv):
    me = greet("feat", n)
    copies = []
    for k in range(1, n):
        copy = pltpu.make_async_remote_copy(
            src_ref=partial_ref,
            dst_ref=held.at[me],
            send_sem=send.at[k - 1],
            recv_sem=recv.at[k - 1],
            device_id={"feat": lax.rem(me + k, n)},
            device_id_type=MESH,
        )
        copy.start()
        copies.append(copy)
    held[me] = partial_ref[...]
    for copy in copies:
        copy.wait()
    margin = held[0]
    for k in range(1, n):
        margin = margin + held[k]
    label = labels_ref[...].astype(jnp.float32)
    residual = 1.0 / (1.0 + jnp.exp(-margin)) - label
    margin_ref[...] = margin
    resid_ref[...] = residual.astype(jnp.bfloat16).astype(jnp.float32)[0:1, :]
    term = jnp.maximum(margin, 0.0) + jnp.log1p(jnp.exp(-jnp.abs(margin))) - label * margin
    total = term[:, 0:LANES]
    for h in range(1, term.shape[1] // LANES):
        total = total + term[:, h * LANES : (h + 1) * LANES]
    loss_ref[...] = total


def gradient_kernel(grains, glist, rlist, nb, resid, idt, vals_ref, out_ref, total):
    total[...] = jnp.zeros_like(total)
    group = lane_group()
    width = GROUP * GRAIN
    per = LANES // GRAIN

    def turn(t, carry):
        base = t * GROUP
        values = group_values(vals_ref, glist, base)
        offset = group_offsets(idt, rlist, base)
        parts = []
        for h in range(GROUP // per):
            row = jnp.zeros((1, LANES), jnp.float32)
            for i in range(per):
                row = jnp.where(group == i, resid[0, glist[base + h * per + i] // grains], row)
            parts.append(row)
        factor = jnp.broadcast_to(jnp.concatenate(parts, axis=1), (8, width))
        for c in range(total.shape[0] // CHUNK):
            spread = jnp.concatenate(
                [jnp.where(offset == c * CHUNK + i * 8, factor, 0.0) for i in range(CHUNK // 8)], axis=0
            ).astype(jnp.bfloat16)
            total[c * CHUNK : (c + 1) * CHUNK, :] += lax.dot_general(
                spread, values, NN, preferred_element_type=jnp.float32
            )
        return carry

    lax.fori_loop(0, nb[0], turn, jnp.int32(0))
    out_ref[...] = total[...].astype(jnp.bfloat16)


def scatter_kernel(n, grad_ref, margin_ref, owner_ref, loss_ref, sum_ref, notes_ref, notes, held, send, recv, nsend, nrecv):
    ex = margin_ref.shape[1]
    rows = sum_ref.shape[0]
    owner = owner_ref[...].astype(jnp.float32)
    square = jnp.broadcast_to(owner, (ex, ex))
    earlier = lax.broadcasted_iota(jnp.int32, (ex, ex), 0) < lax.broadcasted_iota(jnp.int32, (ex, ex), 1)
    same = jnp.where(jnp.logical_and(square.T == square, earlier), 1.0, 0.0)
    rank = jnp.sum(same, axis=0, keepdims=True)
    which = lax.broadcasted_iota(jnp.int32, (n, ex), 0).astype(jnp.float32)
    by_owner = jnp.where(which == owner, margin_ref[0:1, :], 0.0)
    place = lax.broadcasted_iota(jnp.int32, (LANES, ex), 0).astype(jnp.float32)
    by_rank = jnp.where(place == rank, 1.0, 0.0)
    ordered = lax.dot_general(
        by_owner, by_rank, NT, precision=lax.Precision.HIGHEST, preferred_element_type=jnp.float32
    )
    sub = lax.broadcasted_iota(jnp.int32, (8, LANES), 0)
    for d in range(n):
        notes[d] = jnp.where(sub == 0, ordered[d : d + 1, :], loss_ref[...])
    me = greet("rows", n)
    copies = []
    for k in range(1, n):
        peer = lax.rem(me + k, n)
        for source, target, out_sem, in_sem in (
            (grad_ref.at[pl.ds(pl.multiple_of(peer * rows, rows), rows)], held.at[k - 1], send, recv),
            (notes.at[peer], notes_ref.at[me], nsend, nrecv),
        ):
            copy = pltpu.make_async_remote_copy(
                src_ref=source,
                dst_ref=target,
                send_sem=out_sem.at[k - 1],
                recv_sem=in_sem.at[k - 1],
                device_id={"rows": peer},
                device_id_type=MESH,
            )
            copy.start()
            copies.append(copy)
    notes_ref[me] = notes[me]
    sum_ref[...] = grad_ref[pl.ds(pl.multiple_of(me * rows, rows), rows), :].astype(jnp.float32)
    for k in range(1, n):
        copies[2 * k - 2].wait()
        sum_ref[...] += held[k - 1].astype(jnp.float32)
        copies[2 * k - 1].wait()


def on_device(n, nf, tile_values, tile_blocks, tile_counts, labels, owner_rank, weights):
    ex, slots, width = tile_values.shape
    grains = slots // GRAIN
    rows = weights.shape[0]
    f32, i32, bf16 = jnp.float32, jnp.int32, jnp.bfloat16
    shape = jax.ShapeDtypeStruct
    dma = pltpu.SemaphoreType.DMA
    vals = tile_values.reshape(ex * grains, GRAIN, width)

    table = pl.pallas_call(
        functools.partial(gather_kernel, n),
        out_shape=shape((n * rows, width), bf16),
        in_specs=[VM],
        out_specs=VM,
        scratch_shapes=[pltpu.VMEM((rows, width), bf16), dma((n - 1,)), dma((n - 1,))],
        compiler_params=pltpu.CompilerParams(collective_id=0, has_side_effects=True),
    )(weights)

    listed = ex * grains + GROUP
    glist, rlist, nb, idt, partial = pl.pallas_call(
        margin_kernel,
        out_shape=(
            shape((listed,), i32),
            shape((listed,), i32),
            shape((1,), i32),
            shape((ex * grains + 8, LANES), i32),
            shape((8, ex), f32),
        ),
        in_specs=[SM, VM, VM, VM, VM],
        out_specs=(SM, SM, SM, VM, VM),
        scratch_shapes=[pltpu.VMEM((ex * grains + 8, LANES), f32)],
    )(tile_counts.reshape(ex), tile_counts, tile_blocks, table, vals)

    margin, resid, loss_part = pl.pallas_call(
        functools.partial(residual_kernel, nf),
        out_shape=(shape((8, ex), f32), shape((1, ex), f32), shape((8, LANES), f32)),
        in_specs=[VM, VM],
        out_specs=(VM, VM, VM),
        scratch_shapes=[pltpu.VMEM((nf, 8, ex), f32), dma((nf - 1,)), dma((nf - 1,))],
        compiler_params=pltpu.CompilerParams(collective_id=1, has_side_effects=True),
    )(partial, labels.reshape(1, ex))

    grad_part = pl.pallas_call(
        functools.partial(gradient_kernel, grains),
        out_shape=shape((n * rows, width), bf16),
        in_specs=[SM, SM, SM, SM, VM, VM],
        out_specs=VM,
        scratch_shapes=[pltpu.VMEM((n * rows, width), f32)],
    )(glist, rlist, nb, resid, idt, vals)

    gradient, notes = pl.pallas_call(
        functools.partial(scatter_kernel, n),
        out_shape=(shape((rows, width), f32), shape((n, 8, LANES), f32)),
        in_specs=[VM, VM, VM, VM],
        out_specs=(VM, VM),
        scratch_shapes=[
            pltpu.VMEM((n, 8, LANES), f32),
            pltpu.VMEM((n - 1, rows, width), bf16),
            dma((n - 1,)),
            dma((n - 1,)),
            dma((n - 1,)),
            dma((n - 1,)),
        ],
        compiler_params=pltpu.CompilerParams(collective_id=2, has_side_effects=True),
    )(grad_part, margin, owner_rank.reshape(1, ex), loss_part)

    owned_margins = notes[:, 0, : ex // n].reshape(ex)
    loss = jnp.sum(notes[:, 1, :]) / (ex * n)
    return owned_margins, gradient, loss


def solution(mesh):
    in_specs = (
        P("rows", "feat", None),
        P("rows", "feat"),
        P("rows", "feat"),
        P("rows"),
        P("rows"),
        P(("feat", "rows"), None),
    )
    out_specs = (P("rows"), P(("feat", "rows"), None), P())
    body = functools.partial(on_device, mesh.shape["rows"], mesh.shape["feat"])
    return jax.shard_map(body, mesh=mesh, in_specs=in_specs, out_specs=out_specs, check_vma=False)
```

```python
import functools

import jax
import jax.numpy as jnp
from jax import lax
from jax.experimental import pallas as pl
from jax.experimental.pallas import tpu as pltpu
from jax.sharding import PartitionSpec as P

MESH = pl.DeviceIdType.MESH
LANES = 128
GRAIN = 16
GROUP = 16
GRANT = 24 * 1024 * 1024
COST = pl.CostEstimate(flops=0, bytes_accessed=24 * 1024 * 1024, transcendentals=0)
CHUNK = 256
NT = (((1,), (1,)), ((), ()))
NN = (((1,), (0,)), ((), ()))
VM = pl.BlockSpec(memory_space=pltpu.VMEM)
SM = pl.BlockSpec(memory_space=pltpu.SMEM)


def seat(n):
    me = lax.axis_index("rows")
    side = lax.rem(me, 2)
    partner = me + 1 - 2 * side
    column = [lax.rem(me + 2 * k, n) for k in range(n // 2)]
    source = [lax.rem(me + n - 2 * k, n) for k in range(n // 2)]
    return me, partner, column, source


def greet(axis, peers):
    barrier = pltpu.get_barrier_semaphore()
    for peer in peers:
        pl.semaphore_signal(barrier, inc=1, device_id={axis: peer}, device_id_type=MESH)
    pl.semaphore_wait(barrier, len(peers))


def send_to(axis, peer, source, target, send, recv):
    copy = pltpu.make_async_remote_copy(
        src_ref=source,
        dst_ref=target,
        send_sem=send,
        recv_sem=recv,
        device_id={axis: peer},
        device_id_type=MESH,
    )
    copy.start()
    return copy


def gather_kernel(n, w_ref, table_ref, half, send, recv, xsend, xrecv):
    half[...] = w_ref[...].astype(jnp.bfloat16)
    me, partner, column, source = seat(n)
    deep = n // 2
    greet("rows", [partner] + column[1:])
    across = [send_to("rows", partner, half, table_ref.at[me], xsend.at[0], xrecv.at[0])]
    along = [
        send_to("rows", column[k], half, table_ref.at[me], send.at[k - 1], recv.at[k - 1])
        for k in range(1, deep)
    ]
    table_ref[me] = w_ref[...].astype(jnp.bfloat16)
    for k in range(1, deep):
        along[k - 1].wait_recv()
        block = table_ref.at[source[k]]
        across.append(send_to("rows", partner, block, block, xsend.at[k], xrecv.at[k]))
    for copy in along:
        copy.wait_send()
    for copy in across:
        copy.wait()


def lane_group():
    return lax.broadcasted_iota(jnp.int32, (1, LANES), 1) // GRAIN


def group_values(vals_ref, glist, base):
    return jnp.concatenate([vals_ref[glist[base + i]] for i in range(GROUP)], axis=0)


def group_offsets(idt, rlist, base):
    group = lane_group()
    per = LANES // GRAIN
    parts = []
    for h in range(GROUP // per):
        row = idt[pl.ds(rlist[base + h * per], 1), :]
        for i in range(1, per):
            row = jnp.where(group == i, idt[pl.ds(rlist[base + h * per + i], 1), :], row)
        parts.append(row)
    ids = jnp.concatenate(parts, axis=1)
    width = GROUP * GRAIN
    return jnp.broadcast_to(ids, (8, width)) - lax.broadcasted_iota(jnp.int32, (8, width), 0)


def margin_kernel(counts, used_ref, ids_ref, table_ref, vals_ref, glist, rlist, nb, idt, partial_ref, terms):
    slots, ex = ids_ref.shape
    grains = slots // GRAIN
    live = lax.broadcasted_iota(jnp.int32, (slots, ex), 0) < used_ref[...]
    shifted = jnp.where(live, ids_ref[...] + 1, 0)
    if slots < LANES:
        shifted = jnp.concatenate([shifted, jnp.zeros((LANES - slots, ex), jnp.int32)], axis=0)
    shifted = shifted.T
    lane = lax.broadcasted_iota(jnp.int32, (ex, LANES), 1) // GRAIN
    for q in range(grains):
        piece = jnp.where(lane == q, shifted, 0)
        step = GRAIN
        while step < LANES:
            piece = piece + pltpu.roll(piece, step, 1)
            step *= 2
        idt[q * ex : (q + 1) * ex, :] = piece - 1
    idt[grains * ex :, :] = jnp.full((8, LANES), -1, jnp.int32)

    def fill(e, off):
        for q in range(grains):
            glist[off + q] = e * grains + q
            rlist[off + q] = e + q * ex
        return off + (counts[e] + (GRAIN - 1)) // GRAIN

    total = lax.fori_loop(0, ex, fill, jnp.int32(0), unroll=8)
    for i in range(GROUP):
        glist[total + i] = 0
        rlist[total + i] = grains * ex
    turns = (total + (GROUP - 1)) // GROUP
    nb[0] = turns
    terms[...] = jnp.zeros_like(terms)
    group = lane_group()
    width = GROUP * GRAIN
    per = LANES // GRAIN

    def turn(t, carry):
        base = t * GROUP
        values = group_values(vals_ref, glist, base)
        offset = group_offsets(idt, rlist, base)
        found = jnp.zeros((8, width), jnp.float32)
        for c in range(table_ref.shape[0] // CHUNK):
            scores = lax.dot_general(
                table_ref[c * CHUNK : (c + 1) * CHUNK, :], values, NT, preferred_element_type=jnp.float32
            )
            for i in range(CHUNK // 8):
                found = jnp.where(offset == c * CHUNK + i * 8, scores[i * 8 : i * 8 + 8, :], found)
        term = jnp.sum(found, axis=0, keepdims=True)
        for i in range(GROUP):
            h = i // per
            mine = jnp.where(group == i % per, term[:, h * LANES : (h + 1) * LANES], 0.0)
            terms[pl.ds(rlist[base + i], 1), :] = mine
        return carry

    lax.fori_loop(0, turns, turn, jnp.int32(0))
    spread = terms[0:ex, :]
    for q in range(1, grains):
        spread = spread + terms[q * ex : (q + 1) * ex, :]
    partial_ref[...] = jnp.broadcast_to(jnp.sum(spread.T, axis=0, keepdims=True), partial_ref.shape)


def residual_kernel(n, partial_ref, labels_ref, margin_ref, resid_ref, loss_ref, held, send, recv):
    me = lax.axis_index("feat")
    peers = [lax.rem(me + k, n) for k in range(1, n)]
    greet("feat", peers)
    copies = [
        send_to("feat", peer, partial_ref, held.at[me], send.at[k], recv.at[k])
        for k, peer in enumerate(peers)
    ]
    held[me] = partial_ref[...]
    for copy in copies:
        copy.wait()
    margin = held[0]
    for k in range(1, n):
        margin = margin + held[k]
    label = labels_ref[...].astype(jnp.float32)
    residual = 1.0 / (1.0 + jnp.exp(-margin)) - label
    margin_ref[...] = margin
    resid_ref[...] = residual.astype(jnp.bfloat16).astype(jnp.float32)[0:1, :]
    term = jnp.maximum(margin, 0.0) + jnp.log1p(jnp.exp(-jnp.abs(margin))) - label * margin
    total = term[:, 0:LANES]
    for h in range(1, term.shape[1] // LANES):
        total = total + term[:, h * LANES : (h + 1) * LANES]
    loss_ref[...] = total


def gradient_kernel(grains, glist, rlist, nb, resid, idt, vals_ref, out_ref, total):
    total[...] = jnp.zeros_like(total)
    group = lane_group()
    width = GROUP * GRAIN
    per = LANES // GRAIN

    def turn(t, carry):
        base = t * GROUP
        values = group_values(vals_ref, glist, base)
        offset = group_offsets(idt, rlist, base)
        parts = []
        for h in range(GROUP // per):
            row = jnp.zeros((1, LANES), jnp.float32)
            for i in range(per):
                row = jnp.where(group == i, resid[0, glist[base + h * per + i] // grains], row)
            parts.append(row)
        factor = jnp.broadcast_to(jnp.concatenate(parts, axis=1), (8, width))
        for c in range(total.shape[0] // CHUNK):
            spread = jnp.concatenate(
                [jnp.where(offset == c * CHUNK + i * 8, factor, 0.0) for i in range(CHUNK // 8)], axis=0
            ).astype(jnp.bfloat16)
            total[c * CHUNK : (c + 1) * CHUNK, :] += lax.dot_general(
                spread, values, NN, preferred_element_type=jnp.float32
            )
        return carry

    lax.fori_loop(0, nb[0], turn, jnp.int32(0))
    out_ref[...] = total[...].astype(jnp.bfloat16)


def scatter_kernel(n, grad_ref, margin_ref, owner_ref, loss_ref, sum_ref, notes_ref, notes, crossed, paired, held, send, recv, xsend, xrecv, nsend, nrecv):
    ex = margin_ref.shape[1]
    owner = owner_ref[...].astype(jnp.float32)
    square = jnp.broadcast_to(owner, (ex, ex))
    earlier = lax.broadcasted_iota(jnp.int32, (ex, ex), 0) < lax.broadcasted_iota(jnp.int32, (ex, ex), 1)
    same = jnp.where(jnp.logical_and(square.T == square, earlier), 1.0, 0.0)
    rank = jnp.sum(same, axis=0, keepdims=True)
    which = lax.broadcasted_iota(jnp.int32, (n, ex), 0).astype(jnp.float32)
    by_owner = jnp.where(which == owner, margin_ref[0:1, :], 0.0)
    place = lax.broadcasted_iota(jnp.int32, (LANES, ex), 0).astype(jnp.float32)
    by_rank = jnp.where(place == rank, 1.0, 0.0)
    ordered = lax.dot_general(
        by_owner, by_rank, NT, precision=lax.Precision.HIGHEST, preferred_element_type=jnp.float32
    )
    sub = lax.broadcasted_iota(jnp.int32, (8, LANES), 0)
    for d in range(n):
        notes[d] = jnp.where(sub == 0, ordered[d : d + 1, :], loss_ref[...])
    me, partner, column, source = seat(n)
    side = me - partner
    deep = n // 2
    others = [lax.rem(me + k, n) for k in range(1, n)]
    greet("rows", others)
    order = list(range(1, deep)) + [0]
    across = {
        k: send_to("rows", partner, grad_ref.at[column[k] - side], crossed.at[k], xsend.at[k], xrecv.at[k])
        for k in order
    }
    told = [
        send_to("rows", peer, notes.at[peer], notes_ref.at[me], nsend.at[k], nrecv.at[k])
        for k, peer in enumerate(others)
    ]
    notes_ref[me] = notes[me]
    along = []
    for k in range(1, deep):
        across[k].wait_recv()
        pair = grad_ref[column[k]].astype(jnp.float32) + crossed[k].astype(jnp.float32)
        paired[k - 1] = pair.astype(jnp.bfloat16)
        along.append(
            send_to("rows", column[k], paired.at[k - 1], held.at[k - 1], send.at[k - 1], recv.at[k - 1])
        )
    across[0].wait_recv()
    total = grad_ref[me].astype(jnp.float32) + crossed[0].astype(jnp.float32)
    for k in range(1, deep):
        along[k - 1].wait_recv()
        total = total + held[k - 1].astype(jnp.float32)
    sum_ref[...] = total
    for k in order:
        across[k].wait_send()
    for copy in along:
        copy.wait_send()
    for copy in told:
        copy.wait()


def on_device(n, nf, tile_values, tile_blocks, tile_counts, labels, owner_rank, weights):
    ex, slots, width = tile_values.shape
    grains = slots // GRAIN
    rows = weights.shape[0]
    deep = n // 2
    f32, i32, bf16 = jnp.float32, jnp.int32, jnp.bfloat16
    shape = jax.ShapeDtypeStruct
    dma = pltpu.SemaphoreType.DMA
    vals = tile_values.reshape(ex * grains, GRAIN, width)

    table = pl.pallas_call(
        functools.partial(gather_kernel, n),
        out_shape=shape((n, rows, width), bf16),
        in_specs=[VM],
        out_specs=VM,
        scratch_shapes=[pltpu.VMEM((rows, width), bf16), dma((deep - 1,)), dma((deep - 1,)), dma((deep,)), dma((deep,))],
        compiler_params=pltpu.CompilerParams(collective_id=0, has_side_effects=True, vmem_limit_bytes=GRANT),
        cost_estimate=COST,
    )(weights).reshape(n * rows, width)

    listed = ex * grains + GROUP
    glist, rlist, nb, idt, partial = pl.pallas_call(
        margin_kernel,
        out_shape=(
            shape((listed,), i32),
            shape((listed,), i32),
            shape((1,), i32),
            shape((ex * grains + 8, LANES), i32),
            shape((8, ex), f32),
        ),
        in_specs=[SM, VM, VM, VM, VM],
        out_specs=(SM, SM, SM, VM, VM),
        scratch_shapes=[pltpu.VMEM((ex * grains + 8, LANES), f32)],
        compiler_params=pltpu.CompilerParams(vmem_limit_bytes=GRANT),
        cost_estimate=COST,
    )(tile_counts.reshape(ex), tile_counts.reshape(1, ex), tile_blocks.T, table, vals)

    margin, resid, loss_part = pl.pallas_call(
        functools.partial(residual_kernel, nf),
        out_shape=(shape((8, ex), f32), shape((1, ex), f32), shape((8, LANES), f32)),
        in_specs=[VM, VM],
        out_specs=(VM, VM, VM),
        scratch_shapes=[pltpu.VMEM((nf, 8, ex), f32), dma((nf - 1,)), dma((nf - 1,))],
        compiler_params=pltpu.CompilerParams(collective_id=1, has_side_effects=True, vmem_limit_bytes=GRANT),
        cost_estimate=COST,
    )(partial, labels.reshape(1, ex))

    grad_part = pl.pallas_call(
        functools.partial(gradient_kernel, grains),
        out_shape=shape((n * rows, width), bf16),
        in_specs=[SM, SM, SM, SM, VM, VM],
        out_specs=VM,
        scratch_shapes=[pltpu.VMEM((n * rows, width), f32)],
        compiler_params=pltpu.CompilerParams(vmem_limit_bytes=GRANT),
        cost_estimate=COST,
    )(glist, rlist, nb, resid, idt, vals)

    gradient, notes = pl.pallas_call(
        functools.partial(scatter_kernel, n),
        out_shape=(shape((rows, width), f32), shape((n, 8, LANES), f32)),
        in_specs=[VM, VM, VM, VM],
        out_specs=(VM, VM),
        scratch_shapes=[
            pltpu.VMEM((n, 8, LANES), f32),
            pltpu.VMEM((deep, rows, width), bf16),
            pltpu.VMEM((deep - 1, rows, width), bf16),
            pltpu.VMEM((deep - 1, rows, width), bf16),
            dma((deep - 1,)),
            dma((deep - 1,)),
            dma((deep,)),
            dma((deep,)),
            dma((n - 1,)),
            dma((n - 1,)),
        ],
        compiler_params=pltpu.CompilerParams(collective_id=2, has_side_effects=True, vmem_limit_bytes=GRANT),
        cost_estimate=COST,
    )(grad_part.reshape(n, rows, width), margin, owner_rank.reshape(1, ex), loss_part)

    owned_margins = notes[:, 0, : ex // n].reshape(ex)
    loss = jnp.sum(notes[:, 1, :]) / (ex * n)
    return owned_margins, gradient, loss


def solution(mesh):
    in_specs = (
        P("rows", "feat", None),
        P("rows", "feat"),
        P("rows", "feat"),
        P("rows"),
        P("rows"),
        P(("feat", "rows"), None),
    )
    out_specs = (P("rows"), P(("feat", "rows"), None), P())
    body = functools.partial(on_device, mesh.shape["rows"], mesh.shape["feat"])
    return jax.shard_map(body, mesh=mesh, in_specs=in_specs, out_specs=out_specs, check_vma=False)
```

```python
import functools

import jax
import jax.numpy as jnp
from jax import lax
from jax.experimental import pallas as pl
from jax.experimental.pallas import tpu as pltpu
from jax.sharding import PartitionSpec as P

MESH = pl.DeviceIdType.MESH
LANES = 128
GRAIN = 8
GROUP = 32
GRANT = 24 * 1024 * 1024
COST = pl.CostEstimate(flops=0, bytes_accessed=24 * 1024 * 1024, transcendentals=0)
CHUNK = 256
NT = (((1,), (1,)), ((), ()))
NN = (((1,), (0,)), ((), ()))
VM = pl.BlockSpec(memory_space=pltpu.VMEM)
SM = pl.BlockSpec(memory_space=pltpu.SMEM)


def seat(n):
    me = lax.axis_index("rows")
    side = lax.rem(me, 2)
    partner = me + 1 - 2 * side
    column = [lax.rem(me + 2 * k, n) for k in range(n // 2)]
    source = [lax.rem(me + n - 2 * k, n) for k in range(n // 2)]
    return me, partner, column, source


def greet(axis, peers):
    barrier = pltpu.get_barrier_semaphore()
    for peer in peers:
        pl.semaphore_signal(barrier, inc=1, device_id={axis: peer}, device_id_type=MESH)
    pl.semaphore_wait(barrier, len(peers))


def send_to(axis, peer, source, target, send, recv):
    copy = pltpu.make_async_remote_copy(
        src_ref=source,
        dst_ref=target,
        send_sem=send,
        recv_sem=recv,
        device_id={axis: peer},
        device_id_type=MESH,
    )
    copy.start()
    return copy


def gather_kernel(n, w_ref, vals_in, ids_in, used_in, table_ref, vals_ref, ids_ref, used_ref, half, send, recv, xsend, xrecv, lsem):
    half[...] = w_ref[...].astype(jnp.bfloat16)
    me, partner, column, source = seat(n)
    deep = n // 2
    greet("rows", [partner] + column[1:])
    across = [send_to("rows", partner, half, table_ref.at[me], xsend.at[0], xrecv.at[0])]
    along = [
        send_to("rows", column[k], half, table_ref.at[me], send.at[k - 1], recv.at[k - 1])
        for k in range(1, deep)
    ]
    brought = [
        pltpu.make_async_copy(source_ref, target_ref, lsem.at[k])
        for k, (source_ref, target_ref) in enumerate(
            ((ids_in, ids_ref), (used_in, used_ref), (vals_in, vals_ref))
        )
    ]
    for copy in brought:
        copy.start()
    table_ref[me] = w_ref[...].astype(jnp.bfloat16)
    for k in range(1, deep):
        along[k - 1].wait_recv()
        block = table_ref.at[source[k]]
        across.append(send_to("rows", partner, block, block, xsend.at[k], xrecv.at[k]))
    for copy in along:
        copy.wait_send()
    for copy in across + brought:
        copy.wait()


def lane_group():
    return lax.broadcasted_iota(jnp.int32, (1, LANES), 1) // GRAIN


def group_values(vals_ref, glist, base):
    return jnp.concatenate([vals_ref[glist[base + i]] for i in range(GROUP)], axis=0)


def group_offsets(idt, rlist, base):
    group = lane_group()
    per = LANES // GRAIN
    parts = []
    for h in range(GROUP // per):
        row = idt[pl.ds(rlist[base + h * per], 1), :]
        for i in range(1, per):
            row = jnp.where(group == i, idt[pl.ds(rlist[base + h * per + i], 1), :], row)
        parts.append(row)
    ids = jnp.concatenate(parts, axis=1)
    width = GROUP * GRAIN
    return jnp.broadcast_to(ids, (8, width)) - lax.broadcasted_iota(jnp.int32, (8, width), 0)


def margin_kernel(counts, used_ref, ids_ref, table_ref, vals_ref, glist, rlist, nb, idt, partial_ref, terms):
    slots, ex = ids_ref.shape
    grains = slots // GRAIN
    live = lax.broadcasted_iota(jnp.int32, (slots, ex), 0) < used_ref[...]
    shifted = jnp.where(live, ids_ref[...] + 1, 0)
    if slots < LANES:
        shifted = jnp.concatenate([shifted, jnp.zeros((LANES - slots, ex), jnp.int32)], axis=0)
    shifted = shifted.T
    lane = lax.broadcasted_iota(jnp.int32, (ex, LANES), 1) // GRAIN
    for q in range(grains):
        piece = jnp.where(lane == q, shifted, 0)
        step = GRAIN
        while step < LANES:
            piece = piece + pltpu.roll(piece, step, 1)
            step *= 2
        idt[q * ex : (q + 1) * ex, :] = piece - 1
    idt[grains * ex :, :] = jnp.full((8, LANES), -1, jnp.int32)

    def fill(e, off):
        for q in range(grains):
            glist[off + q] = e * grains + q
            rlist[off + q] = e + q * ex
        return off + (counts[e] + (GRAIN - 1)) // GRAIN

    total = lax.fori_loop(0, ex, fill, jnp.int32(0), unroll=8)
    for i in range(GROUP):
        glist[total + i] = 0
        rlist[total + i] = grains * ex
    turns = (total + (GROUP - 1)) // GROUP
    nb[0] = turns
    terms[...] = jnp.zeros_like(terms)
    group = lane_group()
    width = GROUP * GRAIN
    per = LANES // GRAIN

    def turn(t, carry):
        base = t * GROUP
        values = group_values(vals_ref, glist, base)
        offset = group_offsets(idt, rlist, base)
        found = jnp.zeros((8, width), jnp.float32)
        for c in range(table_ref.shape[0] // CHUNK):
            scores = lax.dot_general(
                table_ref[c * CHUNK : (c + 1) * CHUNK, :], values, NT, preferred_element_type=jnp.float32
            )
            for i in range(CHUNK // 8):
                found = jnp.where(offset == c * CHUNK + i * 8, scores[i * 8 : i * 8 + 8, :], found)
        term = jnp.sum(found, axis=0, keepdims=True)
        for i in range(GROUP):
            h = i // per
            mine = jnp.where(group == i % per, term[:, h * LANES : (h + 1) * LANES], 0.0)
            terms[pl.ds(rlist[base + i], 1), :] = mine
        return carry

    lax.fori_loop(0, turns, turn, jnp.int32(0))
    spread = terms[0:ex, :]
    for q in range(1, grains):
        spread = spread + terms[q * ex : (q + 1) * ex, :]
    partial_ref[...] = jnp.broadcast_to(jnp.sum(spread.T, axis=0, keepdims=True), partial_ref.shape)


def residual_kernel(n, partial_ref, labels_ref, margin_ref, resid_ref, loss_ref, held, send, recv):
    me = lax.axis_index("feat")
    peers = [lax.rem(me + k, n) for k in range(1, n)]
    greet("feat", peers)
    copies = [
        send_to("feat", peer, partial_ref, held.at[me], send.at[k], recv.at[k])
        for k, peer in enumerate(peers)
    ]
    held[me] = partial_ref[...]
    for copy in copies:
        copy.wait()
    margin = held[0]
    for k in range(1, n):
        margin = margin + held[k]
    label = labels_ref[...].astype(jnp.float32)
    residual = 1.0 / (1.0 + jnp.exp(-margin)) - label
    margin_ref[...] = margin
    resid_ref[...] = residual.astype(jnp.bfloat16).astype(jnp.float32)[0:1, :]
    term = jnp.maximum(margin, 0.0) + jnp.log1p(jnp.exp(-jnp.abs(margin))) - label * margin
    total = term[:, 0:LANES]
    for h in range(1, term.shape[1] // LANES):
        total = total + term[:, h * LANES : (h + 1) * LANES]
    loss_ref[...] = total


def gradient_kernel(grains, glist, rlist, nb, resid, idt, vals_ref, out_ref, total):
    total[...] = jnp.zeros_like(total)
    group = lane_group()
    width = GROUP * GRAIN
    per = LANES // GRAIN

    def turn(t, carry):
        base = t * GROUP
        values = group_values(vals_ref, glist, base)
        offset = group_offsets(idt, rlist, base)
        parts = []
        for h in range(GROUP // per):
            row = jnp.zeros((1, LANES), jnp.float32)
            for i in range(per):
                row = jnp.where(group == i, resid[0, glist[base + h * per + i] // grains], row)
            parts.append(row)
        factor = jnp.broadcast_to(jnp.concatenate(parts, axis=1), (8, width))
        for c in range(total.shape[0] // CHUNK):
            spread = jnp.concatenate(
                [jnp.where(offset == c * CHUNK + i * 8, factor, 0.0) for i in range(CHUNK // 8)], axis=0
            ).astype(jnp.bfloat16)
            total[c * CHUNK : (c + 1) * CHUNK, :] += lax.dot_general(
                spread, values, NN, preferred_element_type=jnp.float32
            )
        return carry

    lax.fori_loop(0, nb[0], turn, jnp.int32(0))
    out_ref[...] = total[...].astype(jnp.bfloat16)


def scatter_kernel(n, grad_ref, margin_ref, owner_ref, loss_ref, sum_ref, notes_ref, notes, crossed, paired, held, send, recv, xsend, xrecv, nsend, nrecv):
    ex = margin_ref.shape[1]
    owner = owner_ref[...].astype(jnp.float32)
    square = jnp.broadcast_to(owner, (ex, ex))
    earlier = lax.broadcasted_iota(jnp.int32, (ex, ex), 0) < lax.broadcasted_iota(jnp.int32, (ex, ex), 1)
    same = jnp.where(jnp.logical_and(square.T == square, earlier), 1.0, 0.0)
    rank = jnp.sum(same, axis=0, keepdims=True)
    which = lax.broadcasted_iota(jnp.int32, (n, ex), 0).astype(jnp.float32)
    by_owner = jnp.where(which == owner, margin_ref[0:1, :], 0.0)
    place = lax.broadcasted_iota(jnp.int32, (LANES, ex), 0).astype(jnp.float32)
    by_rank = jnp.where(place == rank, 1.0, 0.0)
    ordered = lax.dot_general(
        by_owner, by_rank, NT, precision=lax.Precision.HIGHEST, preferred_element_type=jnp.float32
    )
    sub = lax.broadcasted_iota(jnp.int32, (8, LANES), 0)
    for d in range(n):
        notes[d] = jnp.where(sub == 0, ordered[d : d + 1, :], loss_ref[...])
    me, partner, column, source = seat(n)
    side = me - partner
    deep = n // 2
    others = [lax.rem(me + k, n) for k in range(1, n)]
    greet("rows", others)
    order = list(range(1, deep)) + [0]
    across = {
        k: send_to("rows", partner, grad_ref.at[column[k] - side], crossed.at[k], xsend.at[k], xrecv.at[k])
        for k in order
    }
    told = [
        send_to("rows", peer, notes.at[peer], notes_ref.at[me], nsend.at[k], nrecv.at[k])
        for k, peer in enumerate(others)
    ]
    notes_ref[me] = notes[me]
    along = []
    for k in range(1, deep):
        across[k].wait_recv()
        pair = grad_ref[column[k]].astype(jnp.float32) + crossed[k].astype(jnp.float32)
        paired[k - 1] = pair.astype(jnp.bfloat16)
        along.append(
            send_to("rows", column[k], paired.at[k - 1], held.at[k - 1], send.at[k - 1], recv.at[k - 1])
        )
    across[0].wait_recv()
    total = grad_ref[me].astype(jnp.float32) + crossed[0].astype(jnp.float32)
    for k in range(1, deep):
        along[k - 1].wait_recv()
        total = total + held[k - 1].astype(jnp.float32)
    sum_ref[...] = total
    for k in order:
        across[k].wait_send()
    for copy in along:
        copy.wait_send()
    for copy in told:
        copy.wait()


def on_device(n, nf, tile_values, tile_blocks, tile_counts, labels, owner_rank, weights):
    ex, slots, width = tile_values.shape
    grains = slots // GRAIN
    rows = weights.shape[0]
    deep = n // 2
    f32, i32, bf16 = jnp.float32, jnp.int32, jnp.bfloat16
    shape = jax.ShapeDtypeStruct
    dma = pltpu.SemaphoreType.DMA
    vals = tile_values.reshape(ex * grains, GRAIN, width)

    ANY = pl.BlockSpec(memory_space=pltpu.MemorySpace.HBM)
    table, vals, ids, used = pl.pallas_call(
        functools.partial(gather_kernel, n),
        out_shape=(
            shape((n, rows, width), bf16),
            shape(vals.shape, bf16),
            shape((slots, ex), i32),
            shape((1, ex), i32),
        ),
        in_specs=[VM, ANY, ANY, ANY],
        out_specs=(VM, VM, VM, VM),
        scratch_shapes=[
            pltpu.VMEM((rows, width), bf16),
            dma((deep - 1,)),
            dma((deep - 1,)),
            dma((deep,)),
            dma((deep,)),
            dma((3,)),
        ],
        compiler_params=pltpu.CompilerParams(collective_id=0, has_side_effects=True, vmem_limit_bytes=GRANT),
        cost_estimate=COST,
    )(weights, vals, tile_blocks.T, tile_counts.reshape(1, ex))
    table = table.reshape(n * rows, width)

    listed = ex * grains + GROUP
    glist, rlist, nb, idt, partial = pl.pallas_call(
        margin_kernel,
        out_shape=(
            shape((listed,), i32),
            shape((listed,), i32),
            shape((1,), i32),
            shape((ex * grains + 8, LANES), i32),
            shape((8, ex), f32),
        ),
        in_specs=[SM, VM, VM, VM, VM],
        out_specs=(SM, SM, SM, VM, VM),
        scratch_shapes=[pltpu.VMEM((ex * grains + 8, LANES), f32)],
        compiler_params=pltpu.CompilerParams(vmem_limit_bytes=GRANT),
        cost_estimate=COST,
    )(used.reshape(ex), used, ids, table, vals)

    margin, resid, loss_part = pl.pallas_call(
        functools.partial(residual_kernel, nf),
        out_shape=(shape((8, ex), f32), shape((1, ex), f32), shape((8, LANES), f32)),
        in_specs=[VM, VM],
        out_specs=(VM, VM, VM),
        scratch_shapes=[pltpu.VMEM((nf, 8, ex), f32), dma((nf - 1,)), dma((nf - 1,))],
        compiler_params=pltpu.CompilerParams(collective_id=1, has_side_effects=True, vmem_limit_bytes=GRANT),
        cost_estimate=COST,
    )(partial, labels.reshape(1, ex))

    grad_part = pl.pallas_call(
        functools.partial(gradient_kernel, grains),
        out_shape=shape((n * rows, width), bf16),
        in_specs=[SM, SM, SM, SM, VM, VM],
        out_specs=VM,
        scratch_shapes=[pltpu.VMEM((n * rows, width), f32)],
        compiler_params=pltpu.CompilerParams(vmem_limit_bytes=GRANT),
        cost_estimate=COST,
    )(glist, rlist, nb, resid, idt, vals)

    gradient, notes = pl.pallas_call(
        functools.partial(scatter_kernel, n),
        out_shape=(shape((rows, width), f32), shape((n, 8, LANES), f32)),
        in_specs=[VM, VM, VM, VM],
        out_specs=(VM, VM),
        scratch_shapes=[
            pltpu.VMEM((n, 8, LANES), f32),
            pltpu.VMEM((deep, rows, width), bf16),
            pltpu.VMEM((deep - 1, rows, width), bf16),
            pltpu.VMEM((deep - 1, rows, width), bf16),
            dma((deep - 1,)),
            dma((deep - 1,)),
            dma((deep,)),
            dma((deep,)),
            dma((n - 1,)),
            dma((n - 1,)),
        ],
        compiler_params=pltpu.CompilerParams(collective_id=2, has_side_effects=True, vmem_limit_bytes=GRANT),
        cost_estimate=COST,
    )(grad_part.reshape(n, rows, width), margin, owner_rank.reshape(1, ex), loss_part)

    owned_margins = notes[:, 0, : ex // n].reshape(ex)
    loss = jnp.sum(notes[:, 1, :]) / (ex * n)
    return owned_margins, gradient, loss


def solution(mesh):
    in_specs = (
        P("rows", "feat", None),
        P("rows", "feat"),
        P("rows", "feat"),
        P("rows"),
        P("rows"),
        P(("feat", "rows"), None),
    )
    out_specs = (P("rows"), P(("feat", "rows"), None), P())
    body = functools.partial(on_device, mesh.shape["rows"], mesh.shape["feat"])
    return jax.shard_map(body, mesh=mesh, in_specs=in_specs, out_specs=out_specs, check_vma=False)
```

```python
import functools

import jax
import jax.numpy as jnp
from jax import lax
from jax.experimental import pallas as pl
from jax.experimental.pallas import tpu as pltpu
from jax.sharding import PartitionSpec as P

MESH = pl.DeviceIdType.MESH
LANES = 128
GRAIN = 16
GROUP = 32
GRANT = 24 * 1024 * 1024
COST = pl.CostEstimate(flops=0, bytes_accessed=24 * 1024 * 1024, transcendentals=0)
CHUNK = 256
NT = (((1,), (1,)), ((), ()))
NN = (((1,), (0,)), ((), ()))
VM = pl.BlockSpec(memory_space=pltpu.VMEM)
SM = pl.BlockSpec(memory_space=pltpu.SMEM)


def seat(n):
    me = lax.axis_index("rows")
    side = lax.rem(me, 2)
    partner = me + 1 - 2 * side
    column = [lax.rem(me + 2 * k, n) for k in range(n // 2)]
    source = [lax.rem(me + n - 2 * k, n) for k in range(n // 2)]
    return me, partner, column, source


def greet(axis, peers):
    barrier = pltpu.get_barrier_semaphore()
    for peer in peers:
        pl.semaphore_signal(barrier, inc=1, device_id={axis: peer}, device_id_type=MESH)
    pl.semaphore_wait(barrier, len(peers))


def send_to(axis, peer, source, target, send, recv):
    copy = pltpu.make_async_remote_copy(
        src_ref=source,
        dst_ref=target,
        send_sem=send,
        recv_sem=recv,
        device_id={axis: peer},
        device_id_type=MESH,
    )
    copy.start()
    return copy


def gather_kernel(n, w_ref, table_ref, half, send, recv, xsend, xrecv):
    half[...] = w_ref[...].astype(jnp.bfloat16)
    me, partner, column, source = seat(n)
    deep = n // 2
    greet("rows", [partner] + column[1:])
    across = [send_to("rows", partner, half, table_ref.at[me], xsend.at[0], xrecv.at[0])]
    along = [
        send_to("rows", column[k], half, table_ref.at[me], send.at[k - 1], recv.at[k - 1])
        for k in range(1, deep)
    ]
    table_ref[me] = w_ref[...].astype(jnp.bfloat16)
    for k in range(1, deep):
        along[k - 1].wait_recv()
        block = table_ref.at[source[k]]
        across.append(send_to("rows", partner, block, block, xsend.at[k], xrecv.at[k]))
    for copy in along:
        copy.wait_send()
    for copy in across:
        copy.wait()


def lane_group():
    return lax.broadcasted_iota(jnp.int32, (1, LANES), 1) // GRAIN


def group_values(vals_ref, glist, base):
    return jnp.concatenate([vals_ref[glist[base + i]] for i in range(GROUP)], axis=0)


def group_offsets(idt, rlist, base):
    group = lane_group()
    per = LANES // GRAIN
    parts = []
    for h in range(GROUP // per):
        row = idt[pl.ds(rlist[base + h * per], 1), :]
        for i in range(1, per):
            row = jnp.where(group == i, idt[pl.ds(rlist[base + h * per + i], 1), :], row)
        parts.append(row)
    ids = jnp.concatenate(parts, axis=1)
    width = GROUP * GRAIN
    return jnp.broadcast_to(ids, (8, width)) - lax.broadcasted_iota(jnp.int32, (8, width), 0)


def margin_kernel(counts, used_ref, ids_ref, table_ref, vals_ref, glist, rlist, nb, idt, partial_ref, terms):
    slots, ex = ids_ref.shape
    grains = slots // GRAIN
    live = lax.broadcasted_iota(jnp.int32, (slots, ex), 0) < used_ref[...]
    shifted = jnp.where(live, ids_ref[...] + 1, 0)
    if slots < LANES:
        shifted = jnp.concatenate([shifted, jnp.zeros((LANES - slots, ex), jnp.int32)], axis=0)
    shifted = shifted.T
    lane = lax.broadcasted_iota(jnp.int32, (ex, LANES), 1) // GRAIN
    for q in range(grains):
        piece = jnp.where(lane == q, shifted, 0)
        step = GRAIN
        while step < LANES:
            piece = piece + pltpu.roll(piece, step, 1)
            step *= 2
        idt[q * ex : (q + 1) * ex, :] = piece - 1
    idt[grains * ex :, :] = jnp.full((8, LANES), -1, jnp.int32)

    def fill(e, off):
        for q in range(grains):
            glist[off + q] = e * grains + q
            rlist[off + q] = e + q * ex
        return off + (counts[e] + (GRAIN - 1)) // GRAIN

    total = lax.fori_loop(0, ex, fill, jnp.int32(0), unroll=8)
    for i in range(GROUP):
        glist[total + i] = 0
        rlist[total + i] = grains * ex
    turns = (total + (GROUP - 1)) // GROUP
    nb[0] = turns
    terms[...] = jnp.zeros_like(terms)
    group = lane_group()
    width = GROUP * GRAIN
    per = LANES // GRAIN

    def turn(t, carry):
        base = t * GROUP
        values = group_values(vals_ref, glist, base)
        offset = group_offsets(idt, rlist, base)
        found = jnp.zeros((8, width), jnp.float32)
        for c in range(table_ref.shape[0] // CHUNK):
            scores = lax.dot_general(
                table_ref[c * CHUNK : (c + 1) * CHUNK, :], values, NT, preferred_element_type=jnp.float32
            )
            for i in range(CHUNK // 8):
                found = jnp.where(offset == c * CHUNK + i * 8, scores[i * 8 : i * 8 + 8, :], found)
        term = jnp.sum(found, axis=0, keepdims=True)
        for i in range(GROUP):
            h = i // per
            mine = jnp.where(group == i % per, term[:, h * LANES : (h + 1) * LANES], 0.0)
            terms[pl.ds(rlist[base + i], 1), :] = mine
        return carry

    lax.fori_loop(0, turns, turn, jnp.int32(0))
    spread = terms[0:ex, :]
    for q in range(1, grains):
        spread = spread + terms[q * ex : (q + 1) * ex, :]
    partial_ref[...] = jnp.broadcast_to(jnp.sum(spread.T, axis=0, keepdims=True), partial_ref.shape)


def residual_kernel(n, partial_ref, labels_ref, margin_ref, resid_ref, loss_ref, held, send, recv):
    me = lax.axis_index("feat")
    peers = [lax.rem(me + k, n) for k in range(1, n)]
    greet("feat", peers)
    copies = [
        send_to("feat", peer, partial_ref, held.at[me], send.at[k], recv.at[k])
        for k, peer in enumerate(peers)
    ]
    held[me] = partial_ref[...]
    for copy in copies:
        copy.wait()
    margin = held[0]
    for k in range(1, n):
        margin = margin + held[k]
    label = labels_ref[...].astype(jnp.float32)
    residual = 1.0 / (1.0 + jnp.exp(-margin)) - label
    margin_ref[...] = margin
    resid_ref[...] = residual.astype(jnp.bfloat16).astype(jnp.float32)[0:1, :]
    term = jnp.maximum(margin, 0.0) + jnp.log1p(jnp.exp(-jnp.abs(margin))) - label * margin
    total = term[:, 0:LANES]
    for h in range(1, term.shape[1] // LANES):
        total = total + term[:, h * LANES : (h + 1) * LANES]
    loss_ref[...] = total


def gradient_kernel(grains, glist, rlist, nb, resid, idt, vals_ref, out_ref, total):
    total[...] = jnp.zeros_like(total)
    group = lane_group()
    width = GROUP * GRAIN
    per = LANES // GRAIN

    def turn(t, carry):
        base = t * GROUP
        values = group_values(vals_ref, glist, base)
        offset = group_offsets(idt, rlist, base)
        parts = []
        for h in range(GROUP // per):
            row = jnp.zeros((1, LANES), jnp.float32)
            for i in range(per):
                row = jnp.where(group == i, resid[0, glist[base + h * per + i] // grains], row)
            parts.append(row)
        factor = jnp.broadcast_to(jnp.concatenate(parts, axis=1), (8, width))
        for c in range(total.shape[0] // CHUNK):
            spread = jnp.concatenate(
                [jnp.where(offset == c * CHUNK + i * 8, factor, 0.0) for i in range(CHUNK // 8)], axis=0
            ).astype(jnp.bfloat16)
            total[c * CHUNK : (c + 1) * CHUNK, :] += lax.dot_general(
                spread, values, NN, preferred_element_type=jnp.float32
            )
        return carry

    lax.fori_loop(0, nb[0], turn, jnp.int32(0))
    out_ref[...] = total[...].astype(jnp.bfloat16)


def scatter_kernel(n, grad_ref, margin_ref, owner_ref, loss_ref, sum_ref, notes_ref, notes, crossed, paired, held, send, recv, xsend, xrecv, nsend, nrecv):
    ex = margin_ref.shape[1]
    owner = owner_ref[...].astype(jnp.float32)
    square = jnp.broadcast_to(owner, (ex, ex))
    earlier = lax.broadcasted_iota(jnp.int32, (ex, ex), 0) < lax.broadcasted_iota(jnp.int32, (ex, ex), 1)
    same = jnp.where(jnp.logical_and(square.T == square, earlier), 1.0, 0.0)
    rank = jnp.sum(same, axis=0, keepdims=True)
    which = lax.broadcasted_iota(jnp.int32, (n, ex), 0).astype(jnp.float32)
    by_owner = jnp.where(which == owner, margin_ref[0:1, :], 0.0)
    place = lax.broadcasted_iota(jnp.int32, (LANES, ex), 0).astype(jnp.float32)
    by_rank = jnp.where(place == rank, 1.0, 0.0)
    ordered = lax.dot_general(
        by_owner, by_rank, NT, precision=lax.Precision.HIGHEST, preferred_element_type=jnp.float32
    )
    sub = lax.broadcasted_iota(jnp.int32, (8, LANES), 0)
    for d in range(n):
        notes[d] = jnp.where(sub == 0, ordered[d : d + 1, :], loss_ref[...])
    me, partner, column, source = seat(n)
    side = me - partner
    deep = n // 2
    others = [lax.rem(me + k, n) for k in range(1, n)]
    greet("rows", others)
    order = list(range(1, deep)) + [0]
    across = {
        k: send_to("rows", partner, grad_ref.at[column[k] - side], crossed.at[k], xsend.at[k], xrecv.at[k])
        for k in order
    }
    told = [
        send_to("rows", peer, notes.at[peer], notes_ref.at[me], nsend.at[k], nrecv.at[k])
        for k, peer in enumerate(others)
    ]
    notes_ref[me] = notes[me]
    along = []
    for k in range(1, deep):
        across[k].wait_recv()
        pair = grad_ref[column[k]].astype(jnp.float32) + crossed[k].astype(jnp.float32)
        paired[k - 1] = pair.astype(jnp.bfloat16)
        along.append(
            send_to("rows", column[k], paired.at[k - 1], held.at[k - 1], send.at[k - 1], recv.at[k - 1])
        )
    across[0].wait_recv()
    total = grad_ref[me].astype(jnp.float32) + crossed[0].astype(jnp.float32)
    for k in range(1, deep):
        along[k - 1].wait_recv()
        total = total + held[k - 1].astype(jnp.float32)
    sum_ref[...] = total
    for k in order:
        across[k].wait_send()
    for copy in along:
        copy.wait_send()
    for copy in told:
        copy.wait()


def on_device(n, nf, tile_values, tile_blocks, tile_counts, labels, owner_rank, weights):
    ex, slots, width = tile_values.shape
    grains = slots // GRAIN
    rows = weights.shape[0]
    deep = n // 2
    f32, i32, bf16 = jnp.float32, jnp.int32, jnp.bfloat16
    shape = jax.ShapeDtypeStruct
    dma = pltpu.SemaphoreType.DMA
    vals = tile_values.reshape(ex * grains, GRAIN, width)

    table = pl.pallas_call(
        functools.partial(gather_kernel, n),
        out_shape=shape((n, rows, width), bf16),
        in_specs=[VM],
        out_specs=VM,
        scratch_shapes=[pltpu.VMEM((rows, width), bf16), dma((deep - 1,)), dma((deep - 1,)), dma((deep,)), dma((deep,))],
        compiler_params=pltpu.CompilerParams(collective_id=0, has_side_effects=True, vmem_limit_bytes=GRANT),
        cost_estimate=COST,
    )(weights).reshape(n * rows, width)

    listed = ex * grains + GROUP
    glist, rlist, nb, idt, partial = pl.pallas_call(
        margin_kernel,
        out_shape=(
            shape((listed,), i32),
            shape((listed,), i32),
            shape((1,), i32),
            shape((ex * grains + 8, LANES), i32),
            shape((8, ex), f32),
        ),
        in_specs=[SM, VM, VM, VM, VM],
        out_specs=(SM, SM, SM, VM, VM),
        scratch_shapes=[pltpu.VMEM((ex * grains + 8, LANES), f32)],
        compiler_params=pltpu.CompilerParams(vmem_limit_bytes=GRANT),
        cost_estimate=COST,
    )(tile_counts.reshape(ex), tile_counts.reshape(1, ex), tile_blocks.T, table, vals)

    margin, resid, loss_part = pl.pallas_call(
        functools.partial(residual_kernel, nf),
        out_shape=(shape((8, ex), f32), shape((1, ex), f32), shape((8, LANES), f32)),
        in_specs=[VM, VM],
        out_specs=(VM, VM, VM),
        scratch_shapes=[pltpu.VMEM((nf, 8, ex), f32), dma((nf - 1,)), dma((nf - 1,))],
        compiler_params=pltpu.CompilerParams(collective_id=1, has_side_effects=True, vmem_limit_bytes=GRANT),
        cost_estimate=COST,
    )(partial, labels.reshape(1, ex))

    grad_part = pl.pallas_call(
        functools.partial(gradient_kernel, grains),
        out_shape=shape((n * rows, width), bf16),
        in_specs=[SM, SM, SM, SM, VM, VM],
        out_specs=VM,
        scratch_shapes=[pltpu.VMEM((n * rows, width), f32)],
        compiler_params=pltpu.CompilerParams(vmem_limit_bytes=GRANT),
        cost_estimate=COST,
    )(glist, rlist, nb, resid, idt, vals)

    gradient, notes = pl.pallas_call(
        functools.partial(scatter_kernel, n),
        out_shape=(shape((rows, width), f32), shape((n, 8, LANES), f32)),
        in_specs=[VM, VM, VM, VM],
        out_specs=(VM, VM),
        scratch_shapes=[
            pltpu.VMEM((n, 8, LANES), f32),
            pltpu.VMEM((deep, rows, width), bf16),
            pltpu.VMEM((deep - 1, rows, width), bf16),
            pltpu.VMEM((deep - 1, rows, width), bf16),
            dma((deep - 1,)),
            dma((deep - 1,)),
            dma((deep,)),
            dma((deep,)),
            dma((n - 1,)),
            dma((n - 1,)),
        ],
        compiler_params=pltpu.CompilerParams(collective_id=2, has_side_effects=True, vmem_limit_bytes=GRANT),
        cost_estimate=COST,
    )(grad_part.reshape(n, rows, width), margin, owner_rank.reshape(1, ex), loss_part)

    owned_margins = notes[:, 0, : ex // n].reshape(ex)
    loss = jnp.sum(notes[:, 1, :]) / (ex * n)
    return owned_margins, gradient, loss


def solution(mesh):
    in_specs = (
        P("rows", "feat", None),
        P("rows", "feat"),
        P("rows", "feat"),
        P("rows"),
        P("rows"),
        P(("feat", "rows"), None),
    )
    out_specs = (P("rows"), P(("feat", "rows"), None), P())
    body = functools.partial(on_device, mesh.shape["rows"], mesh.shape["feat"])
    return jax.shard_map(body, mesh=mesh, in_specs=in_specs, out_specs=out_specs, check_vma=False)
```
